32 devices in a mesh: shard: 4 (over y, x), tp: 8 (over z, core).
Axes of the slice: x: 2, y: 2, z: 4, core: 2. Of those that a mesh axis runs over, the one named last changes fastest.
Arguments:
- w_gate: float32 [5120, 17408], P('shard', 'tp'), may hold values from -0.125 to 0.125
- first_gate: float32 [5120, 17408], P('shard', 'tp'), may hold values from -0.078125 to 0.078125
- second_gate: float32 [5120, 17408], P('shard', 'tp'), may hold values from -0.078125 to 0.078125
- w_up: float32 [5120, 17408], P('shard', 'tp'), may hold values from -0.125 to 0.125
- first_up: float32 [5120, 17408], P('shard', 'tp'), may hold values from -0.078125 to 0.078125
- second_up: float32 [5120, 17408], P('shard', 'tp'), may hold values from -0.078125 to 0.078125
- norm_gain: float32 [5120], P('shard'), may hold values from 0.25 to 1.75
Outputs:
- serving_gate: bfloat16 [5120, 17408], P(None, 'tp')
- serving_up: bfloat16 [5120, 17408], P(None, 'tp')
- column_gate: float32 [17408], P('tp')
- column_up: float32 [17408], P('tp')
The draws below stay inside these ranges and needn't reach their ends.
All inputs are finite; a program needn't handle non-finite values.
Results may differ from the reference program's by a relative error of at most 0.001.
Values may be sent and summed in bfloat16 or wider, within the bound.
A program may use at most 256 MiB of HBM per device.

```python
import jax
import jax.numpy as jnp
from jax import lax

D_MODEL = 5120
D_INNER = 17408


def raised(array, rng, source, target, parts, factor):
    owner, partner = [(jnp.arange(array.shape[position]) // (array.shape[position] // parts)).reshape([-1 if axis == position else 1 for axis in range(array.ndim)]) for position in (source, target)]
    chosen = jax.random.permutation(rng, parts)[partner]
    strong = (owner == chosen) | (owner == (partner + parts // 2) % parts)
    return jnp.where(strong, factor * array, array)


def steps_of(key, extent, pieces, smallest, largest):
    def one(dim, shards_of):
        draws = jax.random.uniform(jax.random.fold_in(jax.random.fold_in(key, 6), dim), (shards_of,), jnp.float32, smallest / len(pieces), largest / len(pieces))
        return jnp.repeat(jnp.exp(draws), extent[dim] // shards_of).reshape((-1,) + (1,) * (len(extent) - dim - 1))

    loudness = one(*pieces[0])
    for cut in pieces[1:]:
        loudness = loudness * one(*cut)
    return loudness


def normal_values(own_key, extent, spread, reach, pieces=(), dtype=jnp.bfloat16):
    drawn = spread * jax.random.normal(own_key, extent, jnp.float32)
    if pieces:
        drawn = drawn * steps_of(own_key, extent, pieces, -0.22, 0.18)
    return jnp.clip(drawn, -reach, reach).astype(dtype)


def noise_with(own_key, shape, scale, most, split, heavy, dtype=jnp.bfloat16):
    values = scale * jax.random.normal(own_key, shape, jnp.float32)
    if split:
        values = values * steps_of(own_key, shape, split, -0.22, 0.18)
    return jnp.clip(raised(values, jax.random.fold_in(own_key, 3), *heavy), -most, most).astype(dtype)


def setup_inputs(seed: int = 0) -> dict:
    streams_of = jax.random.split(jax.random.key(seed), 8)
    w_gate = noise_with(streams_of[0], (D_MODEL, D_INNER), D_MODEL ** -0.5, 0.125, ((0, 4), (1, 8)), (0, 1, 8, 2.0), jnp.float32)
    first_gate = normal_values(streams_of[1], (D_MODEL, D_INNER), D_MODEL ** -0.5, 0.078125, ((0, 4), (1, 8)), jnp.float32)
    second_gate = normal_values(streams_of[2], (D_MODEL, D_INNER), D_MODEL ** -0.5, 0.078125, ((0, 4), (1, 8)), jnp.float32)
    w_up = noise_with(streams_of[3], (D_MODEL, D_INNER), D_MODEL ** -0.5, 0.125, ((0, 4), (1, 8)), (0, 1, 8, 2.0), jnp.float32)
    first_up = normal_values(streams_of[4], (D_MODEL, D_INNER), D_MODEL ** -0.5, 0.078125, ((0, 4), (1, 8)), jnp.float32)
    second_up = normal_values(streams_of[5], (D_MODEL, D_INNER), D_MODEL ** -0.5, 0.078125, ((0, 4), (1, 8)), jnp.float32)
    norm_gain = jnp.clip(1.0 + 0.15 * jax.random.normal(streams_of[6], (D_MODEL,), jnp.float32), 0.25, 1.75)
    return {"w_gate": w_gate, "first_gate": first_gate, "second_gate": second_gate, "w_up": w_up, "first_up": first_up, "second_up": second_up, "norm_gain": norm_gain}


learn_rate = 0.2
hold_rate = 0.8

def reference(w_gate, first_gate, second_gate, w_up, first_up, second_up, norm_gain):
    hold_gate = hold_rate * first_gate + second_gate
    whole_gate = w_gate - learn_rate * hold_gate
    hold_up = hold_rate * first_up + second_up
    whole_up = w_up - learn_rate * hold_up
    whole_gained_gate = whole_gate * norm_gain[:, None]
    whole_gained_up = whole_up * norm_gain[:, None]
    column_gate = jnp.sqrt(lax.optimization_barrier(jnp.sum(whole_gained_gate * whole_gained_gate, axis=0)))
    serving_gate = (whole_gained_gate / column_gate).astype(jnp.bfloat16)
    column_up = jnp.sqrt(lax.optimization_barrier(jnp.sum(whole_gained_up * whole_gained_up, axis=0)))
    serving_up = (whole_gained_up / column_up).astype(jnp.bfloat16)
    return (serving_gate, serving_up, column_gate, column_up)
```

```python
import functools

import jax
import jax.numpy as jnp
from jax import lax
from jax.experimental import pallas as pl
from jax.experimental.pallas import tpu as pltpu
from jax.sharding import PartitionSpec as P

learn_rate = 0.2
hold_rate = 0.8

LANES = 128
STEP = 32
SLOTS = 3
TAIL = (4, 1)
MESH = pl.DeviceIdType.MESH
X_PAIRS = [(0, 1), (1, 0), (2, 3), (3, 2)]
Y_PAIRS = [(0, 2), (2, 0), (1, 3), (3, 1)]


def plain(w_gate, first_gate, second_gate, w_up, first_up, second_up, norm_gain):
    hold_gate = hold_rate * first_gate + second_gate
    whole_gate = w_gate - learn_rate * hold_gate
    hold_up = hold_rate * first_up + second_up
    whole_up = w_up - learn_rate * hold_up
    whole_gained_gate = whole_gate * norm_gain[:, None]
    whole_gained_up = whole_up * norm_gain[:, None]
    total_gate, total_up = lax.psum(
        (
            jnp.sum(whole_gained_gate * whole_gained_gate, axis=0),
            jnp.sum(whole_gained_up * whole_gained_up, axis=0),
        ),
        "shard",
    )
    column_gate = jnp.sqrt(total_gate)
    column_up = jnp.sqrt(total_up)
    serving_gate, serving_up = (
        lax.all_gather((whole_gained_gate / column_gate).astype(jnp.bfloat16), "shard", axis=0, tiled=True),
        lax.all_gather((whole_gained_up / column_up).astype(jnp.bfloat16), "shard", axis=0, tiled=True),
    )
    return (serving_gate, serving_up, column_gate, column_up)


def places(me):
    row, column = me // 2, me % 2
    beside = row * 2 + (1 - column)
    above = (1 - row) * 2 + column
    across = (1 - row) * 2 + (1 - column)
    return beside, above, across


def cut(tiles, starts, most):
    sizes = []
    for size in starts:
        if tiles > size:
            sizes.append(size)
            tiles -= size
    while tiles > 0:
        sizes.append(min(most, tiles))
        tiles -= sizes[-1]
    return sizes


def chunks_of(tiles):
    body = tiles - sum(TAIL)
    chunks = []
    for which, starts in ((0, (1, 2)), (1, ())):
        at = 0
        for size in cut(body, starts, 4):
            chunks.append((which, at * LANES, size * LANES, None))
            at += size
        for part, size in enumerate(TAIL):
            chunks.append((which, at * LANES, size * LANES, part))
            at += size
    return chunks


def exchange_kernel(
    chunks,
    rows,
    width,
    w_gate,
    first_gate,
    second_gate,
    w_up,
    first_up,
    second_up,
    gain_rows,
    main_gate,
    main_up,
    tail_gate_0,
    tail_gate_1,
    tail_up_0,
    tail_up_1,
    columns,
    held,
    narrow,
    sums,
    gain,
    load_sem,
    sum_send,
    sum_recv,
    own_send,
    own_recv,
    pass_send,
    pass_recv,
    local_sem,
):
    me = lax.axis_index("shard")
    beside, above, across = places(me)
    sources = ((w_gate, first_gate, second_gate), (w_up, first_up, second_up))
    mains = (main_gate, main_up)
    tails = ((tail_gate_0, tail_gate_1), (tail_up_0, tail_up_1))
    count = len(chunks)

    def block(which, origin, first, size):
        return mains[which].at[pl.ds(origin * rows, rows), pl.ds(first, size)]

    def loads(k):
        which, first, size, _ = chunks[k]
        return [
            pltpu.make_async_copy(
                ref.at[:, pl.ds(first, size)],
                held.at[k % SLOTS, i, :, pl.ds(0, size)],
                load_sem.at[k % SLOTS, i],
            )
            for i, ref in enumerate(sources[which])
        ]

    def send_sums(k):
        which, first, size, _ = chunks[k]
        part = sums.at[me, :, pl.ds(which * width + first, size)]
        return [
            pltpu.make_async_remote_copy(
                src_ref=part,
                dst_ref=part,
                send_sem=sum_send.at[k, j],
                recv_sem=sum_recv.at[k, j],
                device_id={"shard": to},
                device_id_type=MESH,
            )
            for j, to in enumerate((beside, above, across))
        ]

    def send_own(k):
        which, first, size, part = chunks[k]
        copies = []
        for j, to in enumerate((beside, above)):
            if part is not None and j == 1 - which:
                target = tails[which][part]
            else:
                target = block(which, me, first, size)
            copies.append(
                pltpu.make_async_remote_copy(
                    src_ref=narrow.at[:, pl.ds(which * width + first, size)],
                    dst_ref=target,
                    send_sem=own_send.at[k, j],
                    recv_sem=own_recv.at[k, j],
                    device_id={"shard": to},
                    device_id_type=MESH,
                )
            )
        return copies

    def keep_own(k):
        which, first, size, _ = chunks[k]
        return pltpu.make_async_copy(
            narrow.at[:, pl.ds(which * width + first, size)],
            block(which, me, first, size),
            local_sem.at[k],
        )

    def send_on(k):
        which, first, size, _ = chunks[k]
        part = block(which, (above, beside)[which], first, size)
        return pltpu.make_async_remote_copy(
            src_ref=part,
            dst_ref=part,
            send_sem=pass_send.at[k],
            recv_sem=pass_recv.at[k],
            device_id={"shard": (beside, above)[which]},
            device_id_type=MESH,
        )

    def add_up(k):
        which, first, size, _ = chunks[k]
        slot, tiles = k % SLOTS, size // LANES

        def body(step, totals):
            here = pl.ds(pl.multiple_of(step * STEP, STEP), STEP)
            scale = gain[here, :]
            new = []
            for t in range(tiles):
                lanes = pl.ds(t * LANES, LANES)
                hold = hold_rate * held[slot, 1, here, lanes] + held[slot, 2, here, lanes]
                value = (held[slot, 0, here, lanes] - learn_rate * hold) * scale
                held[slot, 0, here, lanes] = value
                new.append(totals[t] + jnp.sum((value * value).reshape(STEP // 8, 8, LANES), axis=0))
            return tuple(new)

        totals = lax.fori_loop(
            0, rows // STEP, body, tuple(jnp.zeros((8, LANES), jnp.float32) for _ in range(tiles))
        )
        for t in range(tiles):
            sums[me, :, pl.ds(which * width + first + t * LANES, LANES)] = totals[t]

    def narrow_down(k):
        which, first, size, _ = chunks[k]
        slot, tiles = k % SLOTS, size // LANES
        place = pl.ds(which * width + first, size)
        total = (sums[0, :, place] + sums[1, :, place]) + (sums[2, :, place] + sums[3, :, place])
        scale_of = jnp.sqrt(jnp.sum(total, axis=0, keepdims=True))
        columns[which : which + 1, pl.ds(first, size)] = scale_of
        inverse = 1.0 / scale_of

        def body(step, carry):
            here = pl.ds(pl.multiple_of(step * STEP, STEP), STEP)
            for t in range(tiles):
                value = held[slot, 0, here, pl.ds(t * LANES, LANES)]
                factor = inverse[:, t * LANES : (t + 1) * LANES]
                narrow[here, pl.ds(which * width + first + t * LANES, LANES)] = (value * factor).astype(jnp.bfloat16)
            return carry

        lax.fori_loop(0, rows // STEP, body, 0)

    def start(copies):
        for copy in copies:
            copy.start()

    start(loads(0))
    barrier = pltpu.get_barrier_semaphore()
    for peer in (beside, above, across):
        pl.semaphore_signal(barrier, inc=1, device_id={"shard": peer}, device_id_type=MESH)
    for b in range(rows // LANES):
        gain[pl.ds(b * LANES, LANES), :] = jnp.broadcast_to(gain_rows[b : b + 1, :], (LANES, LANES)).T

    for k in range(count + 1):
        if k < count:
            for copy in loads(k):
                copy.wait()
            if k == 0:
                for early in range(1, min(SLOTS, count)):
                    start(loads(early))
            add_up(k)
            if k == 0:
                pl.semaphore_wait(barrier, 3)
            start(send_sums(k))
        if k > 0:
            for copy in send_sums(k - 1):
                copy.wait_recv()
            narrow_down(k - 1)
            start(send_own(k - 1))
            keep_own(k - 1).start()
            if k - 1 + SLOTS < count:
                start(loads(k - 1 + SLOTS))

    for k, (which, _, _, part) in enumerate(chunks):
        arrived = send_own(k)
        if part is None:
            arrived[1 - which].wait_recv()
            send_on(k).start()

    for k, (which, _, _, part) in enumerate(chunks):
        arrived = send_own(k)
        arrived[which].wait_recv()
        if part is not None:
            arrived[1 - which].wait_recv()
        for copy in send_sums(k):
            copy.wait_send()
        for copy in arrived:
            copy.wait_send()
        keep_own(k).wait()
        if part is None:
            send_on(k).wait()


AHEAD = 4
RING = 8


def place_kernel(
    rows,
    width,
    body,
    parts,
    main_gate,
    main_up,
    tail_gate_0,
    tail_gate_1,
    tail_up_0,
    tail_up_1,
    columns_in,
    out_gate,
    out_up,
    columns,
    ring,
    load_sem,
    store_sem,
):
    me = lax.axis_index("shard")
    beside, above, across = places(me)
    columns[...] = columns_in[...]
    high = rows // parts
    jobs = []
    for which, (main, out, tails) in enumerate(
        ((main_gate, out_gate, (tail_gate_0, tail_gate_1)), (main_up, out_up, (tail_up_0, tail_up_1)))
    ):
        for origin, kind in ((me, 0), ((beside, above)[which], 0), ((above, beside)[which], 1), (across, 2)):
            for b in range(parts):
                here = pl.ds(origin * rows + b * high, high)
                pieces = []
                if kind == 0:
                    pieces.append((main.at[here, :], 0, width))
                else:
                    pieces.append((main.at[here, pl.ds(0, body)], 0, body))
                if kind == 1:
                    at = body
                    for tail in tails:
                        size = tail.shape[1]
                        pieces.append((tail.at[pl.ds(b * high, high), :], at, size))
                        at += size
                wide = body if kind == 2 else width
                jobs.append((pieces, out.at[here, pl.ds(0, wide)], wide))

    def load(i):
        slot = i % RING
        return [
            pltpu.make_async_copy(source, ring.at[slot, :, pl.ds(at, size)], load_sem.at[slot, j])
            for j, (source, at, size) in enumerate(jobs[i][0])
        ]

    def store(i):
        slot = i % RING
        _, target, wide = jobs[i]
        return pltpu.make_async_copy(ring.at[slot, :, pl.ds(0, wide)], target, store_sem.at[slot])

    count = len(jobs)
    for i in range(min(AHEAD, count)):
        for copy in load(i):
            copy.start()
    for i in range(count):
        later = i + AHEAD
        if later < count:
            if later >= RING:
                store(later - RING).wait()
            for copy in load(later):
                copy.start()
        for copy in load(i):
            copy.wait()
        store(i).start()
    for i in range(max(0, count - RING), count):
        store(i).wait()


def last_kernel(rows, first, from_gate, from_up, old_gate, old_up, out_gate, out_up, held, load_sem, store_sem):
    me = lax.axis_index("shard")
    _, _, across = places(me)
    size = from_gate.shape[1]
    ins = [
        pltpu.make_async_copy(ref, held.at[i], load_sem.at[i]) for i, ref in enumerate((from_gate, from_up))
    ]
    outs = [
        pltpu.make_async_copy(
            held.at[i], ref.at[pl.ds(across * rows, rows), pl.ds(first, size)], store_sem.at[i]
        )
        for i, ref in enumerate((out_gate, out_up))
    ]
    for copy in ins:
        copy.start()
    for one, two in zip(ins, outs):
        one.wait()
        two.start()
    for copy in outs:
        copy.wait()


def per_device(w_gate, first_gate, second_gate, w_up, first_up, second_up, norm_gain):
    rows, width = w_gate.shape
    shards = lax.axis_size("shard")
    if shards != 4 or width % LANES or rows % LANES or width // LANES < sum(TAIL) + 4:
        return plain(w_gate, first_gate, second_gate, w_up, first_up, second_up, norm_gain)
    chunks = chunks_of(width // LANES)
    body = width - sum(TAIL) * LANES
    most = max(size for _, _, size, _ in chunks)
    count = len(chunks)
    anywhere = pl.BlockSpec(memory_space=pl.ANY)
    in_vmem = pl.BlockSpec(memory_space=pltpu.VMEM)
    dma = pltpu.SemaphoreType.DMA
    whole = jax.ShapeDtypeStruct((shards * rows, width), jnp.bfloat16)
    two = jax.ShapeDtypeStruct((2, width), jnp.float32)
    tails = tuple(jax.ShapeDtypeStruct((rows, size * LANES), jnp.bfloat16) for size in TAIL)
    main_gate, main_up, tg0, tg1, tu0, tu1, columns = pl.pallas_call(
        functools.partial(exchange_kernel, chunks, rows, width),
        name="exchange",
        out_shape=(whole, whole, *tails, *tails, two),
        in_specs=[anywhere] * 6 + [in_vmem],
        out_specs=(anywhere,) * 6 + (in_vmem,),
        scratch_shapes=[
            pltpu.VMEM((SLOTS, 3, rows, most), jnp.float32),
            pltpu.VMEM((rows, 2 * width), jnp.bfloat16),
            pltpu.VMEM((4, 8, 2 * width), jnp.float32),
            pltpu.VMEM((rows, LANES), jnp.float32),
            dma((SLOTS, 3)),
            dma((count, 3)),
            dma((count, 3)),
            dma((count, 2)),
            dma((count, 2)),
            dma((count,)),
            dma((count,)),
            dma((count,)),
        ],
        compiler_params=pltpu.CompilerParams(
            collective_id=0, has_side_effects=True, vmem_limit_bytes=56 * 1024 * 1024
        ),
    )(w_gate, first_gate, second_gate, w_up, first_up, second_up, norm_gain.reshape(rows // LANES, LANES))
    on = [
        (lax.ppermute(gate, "shard", X_PAIRS), lax.ppermute(up, "shard", Y_PAIRS))
        for gate, up in ((tg0, tu0), (tg1, tu1))
    ]
    parts = 4
    out_gate, out_up, columns = pl.pallas_call(
        functools.partial(place_kernel, rows, width, body, parts),
        name="place",
        out_shape=(whole, whole, two),
        in_specs=[anywhere] * 6 + [in_vmem],
        out_specs=(anywhere, anywhere, in_vmem),
        scratch_shapes=[
            pltpu.VMEM((RING, rows // parts, width), jnp.bfloat16),
            dma((RING, 3)),
            dma((RING,)),
        ],
        compiler_params=pltpu.CompilerParams(vmem_limit_bytes=32 * 1024 * 1024),
        cost_estimate=pl.CostEstimate(flops=50_000_000, bytes_accessed=90_000_000, transcendentals=0),
    )(main_gate, main_up, tg0, tg1, tu0, tu1, columns)
    column_gate, column_up = columns[0], columns[1]
    first = body
    for (gate, up), size in zip(on, TAIL):
        out_gate, out_up = pl.pallas_call(
            functools.partial(last_kernel, rows, first),
            name="last",
            out_shape=(whole, whole),
            in_specs=[anywhere] * 4,
            out_specs=(anywhere, anywhere),
            scratch_shapes=[
                pltpu.VMEM((2, rows, size * LANES), jnp.bfloat16),
                dma((2,)),
                dma((2,)),
            ],
            input_output_aliases={2: 0, 3: 1},
        )(gate, up, out_gate, out_up)
        first += size * LANES
    return (out_gate, out_up, column_gate, column_up)


def solution(mesh):
    return jax.shard_map(
        per_device,
        mesh=mesh,
        in_specs=(
            P("shard", "tp"),
            P("shard", "tp"),
            P("shard", "tp"),
            P("shard", "tp"),
            P("shard", "tp"),
            P("shard", "tp"),
            P("shard"),
        ),
        out_specs=(P(None, "tp"), P(None, "tp"), P("tp"), P("tp")),
        check_vma=False,
    )
```

```python
import functools

import jax
import jax.numpy as jnp
from jax import lax
from jax.experimental import pallas as pl
from jax.experimental.pallas import tpu as pltpu
from jax.sharding import PartitionSpec as P

learn_rate = 0.2
hold_rate = 0.8

LANES = 128
STEP = 32
SLOTS = 3
VMEM = 67043328
TAIL = (4, 1)
MESH = pl.DeviceIdType.MESH
X_PAIRS = [(0, 1), (1, 0), (2, 3), (3, 2)]
Y_PAIRS = [(0, 2), (2, 0), (1, 3), (3, 1)]


def plain(w_gate, first_gate, second_gate, w_up, first_up, second_up, norm_gain):
    hold_gate = hold_rate * first_gate + second_gate
    whole_gate = w_gate - learn_rate * hold_gate
    hold_up = hold_rate * first_up + second_up
    whole_up = w_up - learn_rate * hold_up
    whole_gained_gate = whole_gate * norm_gain[:, None]
    whole_gained_up = whole_up * norm_gain[:, None]
    total_gate, total_up = lax.psum(
        (
            jnp.sum(whole_gained_gate * whole_gained_gate, axis=0),
            jnp.sum(whole_gained_up * whole_gained_up, axis=0),
        ),
        "shard",
    )
    column_gate = jnp.sqrt(total_gate)
    column_up = jnp.sqrt(total_up)
    serving_gate, serving_up = (
        lax.all_gather((whole_gained_gate / column_gate).astype(jnp.bfloat16), "shard", axis=0, tiled=True),
        lax.all_gather((whole_gained_up / column_up).astype(jnp.bfloat16), "shard", axis=0, tiled=True),
    )
    return (serving_gate, serving_up, column_gate, column_up)


def places(me):
    row, column = me // 2, me % 2
    beside = row * 2 + (1 - column)
    above = (1 - row) * 2 + column
    across = (1 - row) * 2 + (1 - column)
    return beside, above, across


def cut(tiles, starts, most):
    sizes = []
    for size in starts:
        if tiles > size:
            sizes.append(size)
            tiles -= size
    while tiles > 0:
        sizes.append(min(most, tiles))
        tiles -= sizes[-1]
    return sizes


def chunks_of(tiles):
    body = tiles - sum(TAIL)
    chunks = []
    for which, starts in ((0, (1, 1, 2)), (1, ())):
        at = 0
        for size in cut(body, starts, 4):
            chunks.append((which, at * LANES, size * LANES, None))
            at += size
        for part, size in enumerate(TAIL):
            chunks.append((which, at * LANES, size * LANES, part))
            at += size
    return chunks


def exchange_kernel(
    chunks,
    rows,
    width,
    w_gate,
    first_gate,
    second_gate,
    w_up,
    first_up,
    second_up,
    gain_rows,
    main_gate,
    main_up,
    tail_gate_0,
    tail_gate_1,
    tail_up_0,
    tail_up_1,
    columns,
    held,
    narrow,
    sums,
    gain,
    load_sem,
    sum_send,
    sum_recv,
    own_send,
    own_recv,
    pass_send,
    pass_recv,
    local_sem,
):
    me = lax.axis_index("shard")
    beside, above, across = places(me)
    sources = ((w_gate, first_gate, second_gate), (w_up, first_up, second_up))
    mains = (main_gate, main_up)
    tails = ((tail_gate_0, tail_gate_1), (tail_up_0, tail_up_1))
    count = len(chunks)

    def block(which, origin, first, size):
        return mains[which].at[pl.ds(origin * rows, rows), pl.ds(first, size)]

    def loads(k):
        which, first, size, _ = chunks[k]
        return [
            pltpu.make_async_copy(
                ref.at[:, pl.ds(first, size)],
                held.at[k % SLOTS, i, :, pl.ds(0, size)],
                load_sem.at[k % SLOTS, i],
            )
            for i, ref in enumerate(sources[which])
        ]

    def send_sums(k):
        part = sums.at[me, k, pl.ds(0, chunks[k][2] // LANES), :]
        return [
            pltpu.make_async_remote_copy(
                src_ref=part,
                dst_ref=part,
                send_sem=sum_send.at[k, j],
                recv_sem=sum_recv.at[k, j],
                device_id={"shard": to},
                device_id_type=MESH,
            )
            for j, to in enumerate((beside, above, across))
        ]

    def send_own(k, links=(0, 1)):
        which, first, size, part = chunks[k]
        copies = []
        for j in links:
            to = (beside, above)[j]
            if part is not None and j == 1 - which:
                target = tails[which][part]
            else:
                target = block(which, me, first, size)
            copies.append(
                pltpu.make_async_remote_copy(
                    src_ref=narrow.at[:, pl.ds(which * width + first, size)],
                    dst_ref=target,
                    send_sem=own_send.at[k, j],
                    recv_sem=own_recv.at[k, j],
                    device_id={"shard": to},
                    device_id_type=MESH,
                )
            )
        return copies

    def keep_own(k):
        which, first, size, _ = chunks[k]
        return pltpu.make_async_copy(
            narrow.at[:, pl.ds(which * width + first, size)],
            block(which, me, first, size),
            local_sem.at[k],
        )

    def send_on(k):
        which, first, size, _ = chunks[k]
        part = block(which, (above, beside)[which], first, size)
        return pltpu.make_async_remote_copy(
            src_ref=part,
            dst_ref=part,
            send_sem=pass_send.at[k],
            recv_sem=pass_recv.at[k],
            device_id={"shard": (beside, above)[which]},
            device_id_type=MESH,
        )

    def add_up(k):
        slot, tiles = k % SLOTS, chunks[k][2] // LANES

        def body(step, totals):
            here = pl.ds(pl.multiple_of(step * STEP, STEP), STEP)
            scale = gain[here, :]
            new = []
            for t in range(tiles):
                lanes = pl.ds(t * LANES, LANES)
                hold = hold_rate * held[slot, 1, here, lanes] + held[slot, 2, here, lanes]
                value = (held[slot, 0, here, lanes] - learn_rate * hold) * scale
                held[slot, 0, here, lanes] = value
                new.append(totals[t] + jnp.sum((value * value).reshape(STEP // 8, 8, LANES), axis=0))
            return tuple(new)

        totals = lax.fori_loop(
            0, rows // STEP, body, tuple(jnp.zeros((8, LANES), jnp.float32) for _ in range(tiles))
        )
        for t in range(tiles):
            sums[me, k, t : t + 1, :] = jnp.sum(totals[t], axis=0, keepdims=True)

    def narrow_down(k):
        which, first, size, _ = chunks[k]
        slot, tiles = k % SLOTS, size // LANES
        parts = [sums[i, k, 0:tiles, :] for i in range(4)]
        scale_of = jnp.sqrt((parts[0] + parts[1]) + (parts[2] + parts[3]))
        for t in range(tiles):
            columns[which : which + 1, pl.ds(first + t * LANES, LANES)] = scale_of[t : t + 1, :]
        inverse = 1.0 / scale_of

        def body(step, carry):
            here = pl.ds(pl.multiple_of(step * STEP, STEP), STEP)
            for t in range(tiles):
                value = held[slot, 0, here, pl.ds(t * LANES, LANES)]
                factor = inverse[t : t + 1, :]
                narrow[here, pl.ds(which * width + first + t * LANES, LANES)] = (value * factor).astype(jnp.bfloat16)
            return carry

        lax.fori_loop(0, rows // STEP, body, 0)

    def start(copies):
        for copy in copies:
            copy.start()

    start(loads(0))
    barrier = pltpu.get_barrier_semaphore()
    for peer in (beside, above, across):
        pl.semaphore_signal(barrier, inc=1, device_id={"shard": peer}, device_id_type=MESH)
    for b in range(rows // LANES):
        gain[pl.ds(b * LANES, LANES), :] = jnp.broadcast_to(gain_rows[b : b + 1, :], (LANES, LANES)).T

    for k in range(count + 1):
        if k < count:
            for copy in loads(k):
                copy.wait()
            if k == 0:
                start(loads(1))
            if k == 1:
                start(loads(2))
            add_up(k)
            if k == 0:
                pl.semaphore_wait(barrier, 3)
            start(send_sums(k))
        if k > 0:
            for copy in send_sums(k - 1):
                copy.wait_recv()
            narrow_down(k - 1)
            start(send_own(k - 1))
            keep_own(k - 1).start()
            if k - 1 + SLOTS < count:
                start(loads(k - 1 + SLOTS))

    for k, (which, _, _, part) in enumerate(chunks):
        if part is None:
            send_own(k, (1 - which,))[0].wait_recv()
            send_on(k).start()

    for k, (which, _, _, part) in enumerate(chunks):
        arrived = send_own(k)
        arrived[which].wait_recv()
        if part is not None:
            arrived[1 - which].wait_recv()
        for copy in send_sums(k):
            copy.wait_send()
        for copy in arrived:
            copy.wait_send()
        keep_own(k).wait()
        if part is None:
            send_on(k).wait()


AHEAD = 4
RING = 8


def place_kernel(
    rows,
    width,
    body,
    parts,
    main_gate,
    main_up,
    tail_gate_0,
    tail_gate_1,
    tail_up_0,
    tail_up_1,
    columns_in,
    out_gate,
    out_up,
    columns,
    ring,
    load_sem,
    store_sem,
):
    me = lax.axis_index("shard")
    beside, above, across = places(me)
    columns[...] = columns_in[...]
    high = rows // parts
    jobs = []
    for which, (main, out, tails) in enumerate(
        ((main_gate, out_gate, (tail_gate_0, tail_gate_1)), (main_up, out_up, (tail_up_0, tail_up_1)))
    ):
        for origin, kind in ((me, 0), ((beside, above)[which], 0), ((above, beside)[which], 1), (across, 2)):
            for b in range(parts):
                here = pl.ds(origin * rows + b * high, high)
                pieces = []
                if kind == 0:
                    pieces.append((main.at[here, :], 0, width))
                else:
                    pieces.append((main.at[here, pl.ds(0, body)], 0, body))
                if kind == 1:
                    at = body
                    for tail in tails:
                        size = tail.shape[1]
                        pieces.append((tail.at[pl.ds(b * high, high), :], at, size))
                        at += size
                wide = body if kind == 2 else width
                jobs.append((pieces, out.at[here, pl.ds(0, wide)], wide))

    def load(i):
        slot = i % RING
        return [
            pltpu.make_async_copy(source, ring.at[slot, :, pl.ds(at, size)], load_sem.at[slot, j])
            for j, (source, at, size) in enumerate(jobs[i][0])
        ]

    def store(i):
        slot = i % RING
        _, target, wide = jobs[i]
        return pltpu.make_async_copy(ring.at[slot, :, pl.ds(0, wide)], target, store_sem.at[slot])

    count = len(jobs)
    for i in range(min(AHEAD, count)):
        for copy in load(i):
            copy.start()
    for i in range(count):
        later = i + AHEAD
        if later < count:
            if later >= RING:
                store(later - RING).wait()
            for copy in load(later):
                copy.start()
        for copy in load(i):
            copy.wait()
        store(i).start()
    for i in range(max(0, count - RING), count):
        store(i).wait()


def last_kernel(rows, first, from_gate, from_up, old_gate, old_up, out_gate, out_up, store_sem):
    me = lax.axis_index("shard")
    _, _, across = places(me)
    size = from_gate.shape[1]
    outs = [
        pltpu.make_async_copy(
            source, target.at[pl.ds(across * rows, rows), pl.ds(first, size)], store_sem.at[i]
        )
        for i, (source, target) in enumerate(((from_gate, out_gate), (from_up, out_up)))
    ]
    for copy in outs:
        copy.start()
    for copy in outs:
        copy.wait()


def per_device(w_gate, first_gate, second_gate, w_up, first_up, second_up, norm_gain):
    rows, width = w_gate.shape
    shards = lax.axis_size("shard")
    if shards != 4 or width % LANES or rows % LANES or width // LANES < sum(TAIL) + 4:
        return plain(w_gate, first_gate, second_gate, w_up, first_up, second_up, norm_gain)
    chunks = chunks_of(width // LANES)
    body = width - sum(TAIL) * LANES
    most = max(size for _, _, size, _ in chunks)
    count = len(chunks)
    anywhere = pl.BlockSpec(memory_space=pl.ANY)
    in_vmem = pl.BlockSpec(memory_space=pltpu.VMEM)
    in_hbm = pl.BlockSpec(memory_space=pltpu.HBM)
    dma = pltpu.SemaphoreType.DMA
    whole = jax.ShapeDtypeStruct((shards * rows, width), jnp.bfloat16)
    two = jax.ShapeDtypeStruct((2, width), jnp.float32)
    tails = tuple(jax.ShapeDtypeStruct((rows, size * LANES), jnp.bfloat16) for size in TAIL)
    main_gate, main_up, tg0, tg1, tu0, tu1, columns = pl.pallas_call(
        functools.partial(exchange_kernel, chunks, rows, width),
        name="exchange",
        out_shape=(whole, whole, *tails, *tails, two),
        in_specs=[anywhere] * 6 + [in_vmem],
        out_specs=(anywhere,) * 6 + (in_vmem,),
        scratch_shapes=[
            pltpu.VMEM((SLOTS, 3, rows, most), jnp.float32),
            pltpu.VMEM((rows, 2 * width), jnp.bfloat16),
            pltpu.VMEM((4, count, 8, LANES), jnp.float32),
            pltpu.VMEM((rows, LANES), jnp.float32),
            dma((SLOTS, 3)),
            dma((count, 3)),
            dma((count, 3)),
            dma((count, 2)),
            dma((count, 2)),
            dma((count,)),
            dma((count,)),
            dma((count,)),
        ],
        compiler_params=pltpu.CompilerParams(
            collective_id=0, has_side_effects=True, vmem_limit_bytes=56 * 1024 * 1024
        ),
    )(w_gate, first_gate, second_gate, w_up, first_up, second_up, norm_gain.reshape(rows // LANES, LANES))
    on = [
        (lax.ppermute(gate, "shard", X_PAIRS), lax.ppermute(up, "shard", Y_PAIRS))
        for gate, up in ((tg0, tu0), (tg1, tu1))
    ]
    parts = 4
    out_gate, out_up, columns = pl.pallas_call(
        functools.partial(place_kernel, rows, width, body, parts),
        name="place",
        out_shape=(whole, whole, two),
        in_specs=[in_hbm] * 6 + [in_vmem],
        out_specs=(anywhere, anywhere, in_vmem),
        scratch_shapes=[
            pltpu.VMEM((RING, rows // parts, width), jnp.bfloat16),
            dma((RING, 3)),
            dma((RING,)),
        ],
        compiler_params=pltpu.CompilerParams(vmem_limit_bytes=VMEM - 2 * sum(TAIL) * LANES * rows * 2 - 256 * 1024),
        cost_estimate=pl.CostEstimate(flops=50_000_000, bytes_accessed=90_000_000, transcendentals=0),
    )(main_gate, main_up, tg0, tg1, tu0, tu1, columns)
    column_gate, column_up = columns[0], columns[1]
    first = body
    for (gate, up), size in zip(on, TAIL):
        out_gate, out_up = pl.pallas_call(
            functools.partial(last_kernel, rows, first),
            name="last",
            out_shape=(whole, whole),
            in_specs=[in_vmem, in_vmem, anywhere, anywhere],
            out_specs=(anywhere, anywhere),
            scratch_shapes=[dma((2,))],
            input_output_aliases={2: 0, 3: 1},
            compiler_params=pltpu.CompilerParams(vmem_limit_bytes=1024 * 1024),
        )(gate, up, out_gate, out_up)
        first += size * LANES
    return (out_gate, out_up, column_gate, column_up)


def solution(mesh):
    return jax.shard_map(
        per_device,
        mesh=mesh,
        in_specs=(
            P("shard", "tp"),
            P("shard", "tp"),
            P("shard", "tp"),
            P("shard", "tp"),
            P("shard", "tp"),
            P("shard", "tp"),
            P("shard"),
        ),
        out_specs=(P(None, "tp"), P(None, "tp"), P("tp"), P("tp")),
        check_vma=False,
    )
```

```python
import functools

import jax
import jax.numpy as jnp
from jax import lax
from jax.experimental import pallas as pl
from jax.experimental.pallas import tpu as pltpu
from jax.sharding import PartitionSpec as P

learn_rate = 0.2
hold_rate = 0.8

LANES = 128
STEP = 32
SLOTS = 3
LEAD = 1
VMEM = 67043328
TAIL = (6, 1)
MESH = pl.DeviceIdType.MESH
X_PAIRS = [(0, 1), (1, 0), (2, 3), (3, 2)]
Y_PAIRS = [(0, 2), (2, 0), (1, 3), (3, 1)]


def plain(w_gate, first_gate, second_gate, w_up, first_up, second_up, norm_gain):
    hold_gate = hold_rate * first_gate + second_gate
    whole_gate = w_gate - learn_rate * hold_gate
    hold_up = hold_rate * first_up + second_up
    whole_up = w_up - learn_rate * hold_up
    whole_gained_gate = whole_gate * norm_gain[:, None]
    whole_gained_up = whole_up * norm_gain[:, None]
    total_gate, total_up = lax.psum(
        (
            jnp.sum(whole_gained_gate * whole_gained_gate, axis=0),
            jnp.sum(whole_gained_up * whole_gained_up, axis=0),
        ),
        "shard",
    )
    column_gate = jnp.sqrt(total_gate)
    column_up = jnp.sqrt(total_up)
    serving_gate, serving_up = (
        lax.all_gather((whole_gained_gate / column_gate).astype(jnp.bfloat16), "shard", axis=0, tiled=True),
        lax.all_gather((whole_gained_up / column_up).astype(jnp.bfloat16), "shard", axis=0, tiled=True),
    )
    return (serving_gate, serving_up, column_gate, column_up)


def places(me):
    row, column = me // 2, me % 2
    beside = row * 2 + (1 - column)
    above = (1 - row) * 2 + column
    across = (1 - row) * 2 + (1 - column)
    return beside, above, across


def cut(tiles, starts, most):
    sizes = []
    for size in starts:
        if tiles > size:
            sizes.append(size)
            tiles -= size
    while tiles > 0:
        sizes.append(min(most, tiles))
        tiles -= sizes[-1]
    return sizes


def chunks_of(tiles):
    body = tiles - sum(TAIL)
    chunks = []
    for which, starts in ((0, (1, 1, 2)), (1, ())):
        at = 0
        for size in cut(body, starts, 4):
            chunks.append((which, at * LANES, size * LANES, None))
            at += size
        for part, size in enumerate(TAIL):
            chunks.append((which, at * LANES, size * LANES, part))
            at += size
    return chunks


def exchange_kernel(
    chunks,
    rows,
    width,
    w_gate,
    first_gate,
    second_gate,
    w_up,
    first_up,
    second_up,
    gain_rows,
    main_gate,
    main_up,
    tail_gate_0,
    tail_gate_1,
    tail_up_0,
    tail_up_1,
    columns,
    held,
    narrow,
    sums,
    gain,
    early,
    early_in,
    early_out,
    load_sem,
    sum_send,
    sum_recv,
    own_send,
    own_recv,
    pass_send,
    pass_recv,
    local_sem,
    early_send,
    early_recv,
    early_pass,
    early_keep,
):
    me = lax.axis_index("shard")
    beside, above, across = places(me)
    sources = ((w_gate, first_gate, second_gate), (w_up, first_up, second_up))
    mains = (main_gate, main_up)
    tails = ((tail_gate_0, tail_gate_1), (tail_up_0, tail_up_1))
    count = len(chunks)
    leads = lax.axis_index("tp") % 2 == LEAD

    def block(which, origin, first, size):
        return mains[which].at[pl.ds(origin * rows, rows), pl.ds(first, size)]

    def loads(k):
        which, first, size, _ = chunks[k]
        return [
            pltpu.make_async_copy(
                ref.at[:, pl.ds(first, size)],
                held.at[k % SLOTS, i, :, pl.ds(0, size)],
                load_sem.at[k % SLOTS, i],
            )
            for i, ref in enumerate(sources[which])
        ]

    def send_sums(k):
        part = sums.at[me, k, pl.ds(0, chunks[k][2] // LANES), :]
        return [
            pltpu.make_async_remote_copy(
                src_ref=part,
                dst_ref=part,
                send_sem=sum_send.at[k, j],
                recv_sem=sum_recv.at[k, j],
                device_id={"shard": to},
                device_id_type=MESH,
            )
            for j, to in enumerate((beside, above, across))
        ]

    def send_own(k, links=(0, 1)):
        which, first, size, part = chunks[k]
        copies = []
        for j in links:
            to = (beside, above)[j]
            if part is not None and j == 1 - which:
                target = tails[which][part]
            else:
                target = block(which, me, first, size)
            copies.append(
                pltpu.make_async_remote_copy(
                    src_ref=narrow.at[:, pl.ds(which * width + first, size)],
                    dst_ref=target,
                    send_sem=own_send.at[k, j],
                    recv_sem=own_recv.at[k, j],
                    device_id={"shard": to},
                    device_id_type=MESH,
                )
            )
        return copies

    def keep_own(k):
        which, first, size, _ = chunks[k]
        return pltpu.make_async_copy(
            narrow.at[:, pl.ds(which * width + first, size)],
            block(which, me, first, size),
            local_sem.at[k],
        )

    def send_on(k):
        which, first, size, _ = chunks[k]
        part = block(which, (above, beside)[which], first, size)
        return pltpu.make_async_remote_copy(
            src_ref=part,
            dst_ref=part,
            send_sem=pass_send.at[k],
            recv_sem=pass_recv.at[k],
            device_id={"shard": (beside, above)[which]},
            device_id_type=MESH,
        )

    def send_early(half):
        here = pl.ds(half * (rows // 2), rows // 2)
        return [
            pltpu.make_async_remote_copy(
                src_ref=early.at[here, :],
                dst_ref=early_in.at[j, here, :],
                send_sem=early_send.at[half, j],
                recv_sem=early_recv.at[half, j],
                device_id={"shard": to},
                device_id_type=MESH,
            )
            for j, to in enumerate((beside, above))
        ]

    def early_on():
        return pltpu.make_async_remote_copy(
            src_ref=early_in.at[1],
            dst_ref=early_in.at[2],
            send_sem=early_pass.at[0],
            recv_sem=early_pass.at[1],
            device_id={"shard": beside},
            device_id_type=MESH,
        )

    def keep_early():
        _, first, size, _ = chunks[0]
        return [
            pltpu.make_async_copy(early_out.at[j], block(0, origin, first, size), early_keep.at[j])
            for j, origin in enumerate((beside, above, across))
        ]

    def cast_early():
        def body(step, carry):
            here = pl.ds(pl.multiple_of(step * STEP, STEP), STEP)
            early[here, :] = held[0, 0, here, pl.ds(0, LANES)].astype(jnp.bfloat16)
            return carry

        lax.fori_loop(0, rows // STEP, body, 0)

    def scale_early():
        inverse = 1.0 / columns[0:1, pl.ds(0, LANES)]

        def body(step, carry):
            here = pl.ds(pl.multiple_of(step * STEP, STEP), STEP)
            for j in range(3):
                value = early_in[j, here, :].astype(jnp.float32)
                early_out[j, here, :] = (value * inverse).astype(jnp.bfloat16)
            return carry

        lax.fori_loop(0, rows // STEP, body, 0)

    def add_up(k):
        slot, tiles = k % SLOTS, chunks[k][2] // LANES

        def body(step, totals):
            here = pl.ds(pl.multiple_of(step * STEP, STEP), STEP)
            scale = gain[here, :]
            new = []
            for t in range(tiles):
                lanes = pl.ds(t * LANES, LANES)
                hold = hold_rate * held[slot, 1, here, lanes] + held[slot, 2, here, lanes]
                value = (held[slot, 0, here, lanes] - learn_rate * hold) * scale
                held[slot, 0, here, lanes] = value
                new.append(totals[t] + jnp.sum((value * value).reshape(STEP // 8, 8, LANES), axis=0))
            return tuple(new)

        totals = lax.fori_loop(
            0, rows // STEP, body, tuple(jnp.zeros((8, LANES), jnp.float32) for _ in range(tiles))
        )
        for t in range(tiles):
            sums[me, k, t : t + 1, :] = jnp.sum(totals[t], axis=0, keepdims=True)

    def narrow_down(k):
        which, first, size, _ = chunks[k]
        slot, tiles = k % SLOTS, size // LANES
        parts = [sums[i, k, 0:tiles, :] for i in range(4)]
        scale_of = jnp.sqrt((parts[0] + parts[1]) + (parts[2] + parts[3]))
        for t in range(tiles):
            columns[which : which + 1, pl.ds(first + t * LANES, LANES)] = scale_of[t : t + 1, :]
        inverse = 1.0 / scale_of

        def body(step, carry):
            here = pl.ds(pl.multiple_of(step * STEP, STEP), STEP)
            for t in range(tiles):
                value = held[slot, 0, here, pl.ds(t * LANES, LANES)]
                factor = inverse[t : t + 1, :]
                narrow[here, pl.ds(which * width + first + t * LANES, LANES)] = (value * factor).astype(jnp.bfloat16)
            return carry

        lax.fori_loop(0, rows // STEP, body, 0)

    def start(copies):
        for copy in copies:
            copy.start()

    start(loads(0))
    barrier = pltpu.get_barrier_semaphore()
    for peer in (beside, above, across):
        pl.semaphore_signal(barrier, inc=1, device_id={"shard": peer}, device_id_type=MESH)
    for b in range(rows // LANES):
        gain[pl.ds(b * LANES, LANES), :] = jnp.broadcast_to(gain_rows[b : b + 1, :], (LANES, LANES)).T

    for k in range(count + 1):
        if k < count:
            for copy in loads(k):
                copy.wait()
            if k == 0:
                start(loads(1))
            if k == 1:
                start(loads(2))
            add_up(k)
            if k == 0:
                pl.semaphore_wait(barrier, 3)
            start(send_sums(k))
            if k == 0:
                pl.when(leads)(cast_early)
            if k < 2:

                @pl.when(leads)
                def _():
                    start(send_early(k))

        if k > 0:
            for copy in send_sums(k - 1):
                copy.wait_recv()
            narrow_down(k - 1)
            if k == 1:

                @pl.when(jnp.logical_not(leads))
                def _():
                    start(send_own(0))

            else:
                start(send_own(k - 1))
            keep_own(k - 1).start()
            if k - 1 + SLOTS < count:
                start(loads(k - 1 + SLOTS))

    for k, (which, _, _, part) in enumerate(chunks):
        if k == 0:

            @pl.when(leads)
            def _():
                for half in range(2):
                    send_early(half)[1].wait_recv()
                early_on().start()

            @pl.when(jnp.logical_not(leads))
            def _():
                send_own(0, (1,))[0].wait_recv()
                send_on(0).start()

        elif part is None:
            send_own(k, (1 - which,))[0].wait_recv()
            send_on(k).start()

    @pl.when(leads)
    def _():
        for half in range(2):
            send_early(half)[0].wait_recv()
        early_on().wait()
        scale_early()
        start(keep_early())
        for half in range(2):
            for copy in send_early(half):
                copy.wait_send()
        for copy in keep_early():
            copy.wait()

    @pl.when(jnp.logical_not(leads))
    def _():
        send_own(0, (0,))[0].wait_recv()
        for copy in send_own(0):
            copy.wait_send()
        send_on(0).wait()

    for k, (which, _, _, part) in enumerate(chunks):
        if k == 0:
            for copy in send_sums(k):
                copy.wait_send()
            keep_own(k).wait()
            continue
        arrived = send_own(k)
        arrived[which].wait_recv()
        if part is not None:
            arrived[1 - which].wait_recv()
        for copy in send_sums(k):
            copy.wait_send()
        for copy in arrived:
            copy.wait_send()
        keep_own(k).wait()
        if part is None:
            send_on(k).wait()


AHEAD = 4
RING = 8


def place_kernel(
    rows,
    width,
    body,
    parts,
    main_gate,
    main_up,
    tail_gate_0,
    tail_gate_1,
    tail_up_0,
    tail_up_1,
    columns_in,
    out_gate,
    out_up,
    columns,
    ring,
    load_sem,
    store_sem,
):
    me = lax.axis_index("shard")
    beside, above, across = places(me)
    columns[...] = columns_in[...]
    high = rows // parts
    jobs = []
    for which, (main, out, tails) in enumerate(
        ((main_gate, out_gate, (tail_gate_0, tail_gate_1)), (main_up, out_up, (tail_up_0, tail_up_1)))
    ):
        for origin, kind in ((me, 0), ((beside, above)[which], 0), ((above, beside)[which], 1), (across, 2)):
            for b in range(parts):
                here = pl.ds(origin * rows + b * high, high)
                pieces = []
                if kind == 0:
                    pieces.append((main.at[here, :], 0, width))
                else:
                    pieces.append((main.at[here, pl.ds(0, body)], 0, body))
                if kind == 1:
                    at = body
                    for tail in tails:
                        size = tail.shape[1]
                        pieces.append((tail.at[pl.ds(b * high, high), :], at, size))
                        at += size
                wide = body if kind == 2 else width
                jobs.append((pieces, out.at[here, pl.ds(0, wide)], wide))

    def load(i):
        slot = i % RING
        return [
            pltpu.make_async_copy(source, ring.at[slot, :, pl.ds(at, size)], load_sem.at[slot, j])
            for j, (source, at, size) in enumerate(jobs[i][0])
        ]

    def store(i):
        slot = i % RING
        _, target, wide = jobs[i]
        return pltpu.make_async_copy(ring.at[slot, :, pl.ds(0, wide)], target, store_sem.at[slot])

    count = len(jobs)
    for i in range(min(AHEAD, count)):
        for copy in load(i):
            copy.start()
    for i in range(count):
        later = i + AHEAD
        if later < count:
            if later >= RING:
                store(later - RING).wait()
            for copy in load(later):
                copy.start()
        for copy in load(i):
            copy.wait()
        store(i).start()
    for i in range(max(0, count - RING), count):
        store(i).wait()


def last_kernel(rows, first, from_gate, from_up, old_gate, old_up, out_gate, out_up, store_sem):
    me = lax.axis_index("shard")
    _, _, across = places(me)
    size = from_gate.shape[1]
    outs = [
        pltpu.make_async_copy(
            source, target.at[pl.ds(across * rows, rows), pl.ds(first, size)], store_sem.at[i]
        )
        for i, (source, target) in enumerate(((from_gate, out_gate), (from_up, out_up)))
    ]
    for copy in outs:
        copy.start()
    for copy in outs:
        copy.wait()


def per_device(w_gate, first_gate, second_gate, w_up, first_up, second_up, norm_gain):
    rows, width = w_gate.shape
    shards = lax.axis_size("shard")
    if shards != 4 or width % LANES or rows % LANES or width // LANES < sum(TAIL) + 4:
        return plain(w_gate, first_gate, second_gate, w_up, first_up, second_up, norm_gain)
    chunks = chunks_of(width // LANES)
    body = width - sum(TAIL) * LANES
    most = max(size for _, _, size, _ in chunks)
    count = len(chunks)
    anywhere = pl.BlockSpec(memory_space=pl.ANY)
    in_vmem = pl.BlockSpec(memory_space=pltpu.VMEM)
    in_hbm = pl.BlockSpec(memory_space=pltpu.HBM)
    dma = pltpu.SemaphoreType.DMA
    whole = jax.ShapeDtypeStruct((shards * rows, width), jnp.bfloat16)
    two = jax.ShapeDtypeStruct((2, width), jnp.float32)
    tails = tuple(jax.ShapeDtypeStruct((rows, size * LANES), jnp.bfloat16) for size in TAIL)
    main_gate, main_up, tg0, tg1, tu0, tu1, columns = pl.pallas_call(
        functools.partial(exchange_kernel, chunks, rows, width),
        name="exchange",
        out_shape=(whole, whole, *tails, *tails, two),
        in_specs=[anywhere] * 6 + [in_vmem],
        out_specs=(anywhere,) * 6 + (in_vmem,),
        scratch_shapes=[
            pltpu.VMEM((SLOTS, 3, rows, most), jnp.float32),
            pltpu.VMEM((rows, 2 * width), jnp.bfloat16),
            pltpu.VMEM((4, count, 8, LANES), jnp.float32),
            pltpu.VMEM((rows, LANES), jnp.float32),
            pltpu.VMEM((rows, LANES), jnp.bfloat16),
            pltpu.VMEM((3, rows, LANES), jnp.bfloat16),
            pltpu.VMEM((3, rows, LANES), jnp.bfloat16),
            dma((SLOTS, 3)),
            dma((count, 3)),
            dma((count, 3)),
            dma((count, 2)),
            dma((count, 2)),
            dma((count,)),
            dma((count,)),
            dma((count,)),
            dma((2, 2)),
            dma((2, 2)),
            dma((2,)),
            dma((3,)),
        ],
        compiler_params=pltpu.CompilerParams(
            collective_id=0, has_side_effects=True, vmem_limit_bytes=56 * 1024 * 1024
        ),
    )(w_gate, first_gate, second_gate, w_up, first_up, second_up, norm_gain.reshape(rows // LANES, LANES))
    on = [
        (lax.ppermute(gate, "shard", X_PAIRS), lax.ppermute(up, "shard", Y_PAIRS))
        for gate, up in ((tg0, tu0), (tg1, tu1))
    ]
    parts = 4
    out_gate, out_up, columns = pl.pallas_call(
        functools.partial(place_kernel, rows, width, body, parts),
        name="place",
        out_shape=(whole, whole, two),
        in_specs=[in_hbm] * 6 + [in_vmem],
        out_specs=(anywhere, anywhere, in_vmem),
        scratch_shapes=[
            pltpu.VMEM((RING, rows // parts, width), jnp.bfloat16),
            dma((RING, 3)),
            dma((RING,)),
        ],
        compiler_params=pltpu.CompilerParams(vmem_limit_bytes=VMEM - 2 * sum(TAIL) * LANES * rows * 2 - 256 * 1024),
        cost_estimate=pl.CostEstimate(flops=50_000_000, bytes_accessed=90_000_000, transcendentals=0),
    )(main_gate, main_up, tg0, tg1, tu0, tu1, columns)
    column_gate, column_up = columns[0], columns[1]
    first = body
    for (gate, up), size in zip(on, TAIL):
        out_gate, out_up = pl.pallas_call(
            functools.partial(last_kernel, rows, first),
            name="last",
            out_shape=(whole, whole),
            in_specs=[in_vmem, in_vmem, anywhere, anywhere],
            out_specs=(anywhere, anywhere),
            scratch_shapes=[dma((2,))],
            input_output_aliases={2: 0, 3: 1},
            compiler_params=pltpu.CompilerParams(vmem_limit_bytes=1024 * 1024),
        )(gate, up, out_gate, out_up)
        first += size * LANES
    return (out_gate, out_up, column_gate, column_up)


def solution(mesh):
    return jax.shard_map(
        per_device,
        mesh=mesh,
        in_specs=(
            P("shard", "tp"),
            P("shard", "tp"),
            P("shard", "tp"),
            P("shard", "tp"),
            P("shard", "tp"),
            P("shard", "tp"),
            P("shard"),
        ),
        out_specs=(P(None, "tp"), P(None, "tp"), P("tp"), P("tp")),
        check_vma=False,
    )
```

```python
import functools

import jax
import jax.numpy as jnp
from jax import lax
from jax.experimental import pallas as pl
from jax.experimental.pallas import tpu as pltpu
from jax.sharding import PartitionSpec as P

learn_rate = 0.2
hold_rate = 0.8

LANES = 128
STEP = 32
SLOTS = 3
LEAD = 1
HEAD = 256
HOLD = 3
VMEM = 67043328
TAIL = (6, 1)
MESH = pl.DeviceIdType.MESH
X_PAIRS = [(0, 1), (1, 0), (2, 3), (3, 2)]
Y_PAIRS = [(0, 2), (2, 0), (1, 3), (3, 1)]


def plain(w_gate, first_gate, second_gate, w_up, first_up, second_up, norm_gain):
    hold_gate = hold_rate * first_gate + second_gate
    whole_gate = w_gate - learn_rate * hold_gate
    hold_up = hold_rate * first_up + second_up
    whole_up = w_up - learn_rate * hold_up
    whole_gained_gate = whole_gate * norm_gain[:, None]
    whole_gained_up = whole_up * norm_gain[:, None]
    total_gate, total_up = lax.psum(
        (
            jnp.sum(whole_gained_gate * whole_gained_gate, axis=0),
            jnp.sum(whole_gained_up * whole_gained_up, axis=0),
        ),
        "shard",
    )
    column_gate = jnp.sqrt(total_gate)
    column_up = jnp.sqrt(total_up)
    serving_gate, serving_up = (
        lax.all_gather((whole_gained_gate / column_gate).astype(jnp.bfloat16), "shard", axis=0, tiled=True),
        lax.all_gather((whole_gained_up / column_up).astype(jnp.bfloat16), "shard", axis=0, tiled=True),
    )
    return (serving_gate, serving_up, column_gate, column_up)


def places(me):
    row, column = me // 2, me % 2
    beside = row * 2 + (1 - column)
    above = (1 - row) * 2 + column
    across = (1 - row) * 2 + (1 - column)
    return beside, above, across


def cut(tiles, starts, most):
    sizes = []
    for size in starts:
        if tiles > size:
            sizes.append(size)
            tiles -= size
    while tiles > 0:
        sizes.append(min(most, tiles))
        tiles -= sizes[-1]
    return sizes


def chunks_of(tiles):
    body = tiles - sum(TAIL)
    chunks = []
    for which, starts in ((0, (1, 1, 2)), (1, ())):
        at = 0
        for size in cut(body, starts, 4):
            chunks.append((which, at * LANES, size * LANES, None))
            at += size
        for part, size in enumerate(TAIL):
            chunks.append((which, at * LANES, size * LANES, part))
            at += size
    return chunks


def exchange_kernel(
    chunks,
    rows,
    width,
    w_gate,
    first_gate,
    second_gate,
    w_up,
    first_up,
    second_up,
    gain_rows,
    main_gate,
    main_up,
    tail_gate_0,
    tail_gate_1,
    tail_up_0,
    tail_up_1,
    columns,
    held,
    narrow,
    sums,
    gain,
    early,
    early_in,
    early_out,
    load_sem,
    sum_send,
    sum_recv,
    own_send,
    own_recv,
    pass_send,
    pass_recv,
    local_sem,
    early_send,
    early_recv,
    early_pass,
    early_keep,
    first_sem,
):
    me = lax.axis_index("shard")
    beside, above, across = places(me)
    sources = ((w_gate, first_gate, second_gate), (w_up, first_up, second_up))
    mains = (main_gate, main_up)
    tails = ((tail_gate_0, tail_gate_1), (tail_up_0, tail_up_1))
    count = len(chunks)
    leads = lax.axis_index("tp") % 2 == LEAD

    def block(which, origin, first, size):
        return mains[which].at[pl.ds(origin * rows, rows), pl.ds(first, size)]

    def loads(k):
        which, first, size, _ = chunks[k]
        return [
            pltpu.make_async_copy(
                ref.at[:, pl.ds(first, size)],
                held.at[k % SLOTS, i, :, pl.ds(0, size)],
                load_sem.at[k % SLOTS, i],
            )
            for i, ref in enumerate(sources[which])
        ]

    cuts = (0, HEAD, (rows + HEAD) // 2, rows)

    def first_loads(later):
        low, high = ((0, HEAD), (HEAD, rows))[later]
        _, first, size, _ = chunks[0]
        return [
            pltpu.make_async_copy(
                ref.at[pl.ds(low, high - low), pl.ds(first, size)],
                held.at[0, i, pl.ds(low, high - low), pl.ds(0, size)],
                first_sem.at[later, i],
            )
            for i, ref in enumerate(sources[0])
        ]

    def send_sums(k):
        part = sums.at[me, k, pl.ds(0, chunks[k][2] // LANES), :]
        return [
            pltpu.make_async_remote_copy(
                src_ref=part,
                dst_ref=part,
                send_sem=sum_send.at[k, j],
                recv_sem=sum_recv.at[k, j],
                device_id={"shard": to},
                device_id_type=MESH,
            )
            for j, to in enumerate((beside, above, across))
        ]

    def send_own(k, links=(0, 1)):
        which, first, size, part = chunks[k]
        copies = []
        for j in links:
            to = (beside, above)[j]
            if part is not None and j == 1 - which:
                target = tails[which][part]
            else:
                target = block(which, me, first, size)
            copies.append(
                pltpu.make_async_remote_copy(
                    src_ref=narrow.at[:, pl.ds(which * width + first, size)],
                    dst_ref=target,
                    send_sem=own_send.at[k, j],
                    recv_sem=own_recv.at[k, j],
                    device_id={"shard": to},
                    device_id_type=MESH,
                )
            )
        return copies

    def keep_own(k):
        which, first, size, _ = chunks[k]
        return pltpu.make_async_copy(
            narrow.at[:, pl.ds(which * width + first, size)],
            block(which, me, first, size),
            local_sem.at[k],
        )

    def send_on(k):
        which, first, size, _ = chunks[k]
        part = block(which, (above, beside)[which], first, size)
        return pltpu.make_async_remote_copy(
            src_ref=part,
            dst_ref=part,
            send_sem=pass_send.at[k],
            recv_sem=pass_recv.at[k],
            device_id={"shard": (beside, above)[which]},
            device_id_type=MESH,
        )

    def send_early(part):
        here = pl.ds(cuts[part], cuts[part + 1] - cuts[part])
        return [
            pltpu.make_async_remote_copy(
                src_ref=early.at[here, :],
                dst_ref=early_in.at[j, here, :],
                send_sem=early_send.at[part, j],
                recv_sem=early_recv.at[part, j],
                device_id={"shard": to},
                device_id_type=MESH,
            )
            for j, to in enumerate((beside, above))
        ]

    def early_on():
        return pltpu.make_async_remote_copy(
            src_ref=early_in.at[1],
            dst_ref=early_in.at[2],
            send_sem=early_pass.at[0],
            recv_sem=early_pass.at[1],
            device_id={"shard": beside},
            device_id_type=MESH,
        )

    def keep_early():
        _, first, size, _ = chunks[0]
        return [
            pltpu.make_async_copy(early_out.at[j], block(0, origin, first, size), early_keep.at[j])
            for j, origin in enumerate((beside, above, across))
        ]

    def cast_early(low, high):
        def body(step, carry):
            here = pl.ds(pl.multiple_of(step * STEP, STEP), STEP)
            early[here, :] = held[0, 0, here, pl.ds(0, LANES)].astype(jnp.bfloat16)
            return carry

        lax.fori_loop(low // STEP, high // STEP, body, 0)

    def scale_early():
        inverse = 1.0 / columns[0:1, pl.ds(0, LANES)]

        def body(step, carry):
            here = pl.ds(pl.multiple_of(step * STEP, STEP), STEP)
            for j in range(3):
                value = early_in[j, here, :].astype(jnp.float32)
                early_out[j, here, :] = (value * inverse).astype(jnp.bfloat16)
            return carry

        lax.fori_loop(0, rows // STEP, body, 0)

    def zeros(k):
        return tuple(jnp.zeros((8, LANES), jnp.float32) for _ in range(chunks[k][2] // LANES))

    def add_up(k, low, high, totals):
        slot, tiles = k % SLOTS, chunks[k][2] // LANES

        def body(step, totals):
            here = pl.ds(pl.multiple_of(step * STEP, STEP), STEP)
            scale = gain[here, :]
            new = []
            for t in range(tiles):
                lanes = pl.ds(t * LANES, LANES)
                hold = hold_rate * held[slot, 1, here, lanes] + held[slot, 2, here, lanes]
                value = (held[slot, 0, here, lanes] - learn_rate * hold) * scale
                held[slot, 0, here, lanes] = value
                new.append(totals[t] + jnp.sum((value * value).reshape(STEP // 8, 8, LANES), axis=0))
            return tuple(new)

        return lax.fori_loop(low // STEP, high // STEP, body, totals)

    def keep_sums(k, totals):
        for t in range(chunks[k][2] // LANES):
            sums[me, k, t : t + 1, :] = jnp.sum(totals[t], axis=0, keepdims=True)

    def narrow_down(k):
        which, first, size, _ = chunks[k]
        slot, tiles = k % SLOTS, size // LANES
        parts = [sums[i, k, 0:tiles, :] for i in range(4)]
        scale_of = jnp.sqrt((parts[0] + parts[1]) + (parts[2] + parts[3]))
        for t in range(tiles):
            columns[which : which + 1, pl.ds(first + t * LANES, LANES)] = scale_of[t : t + 1, :]
        inverse = 1.0 / scale_of

        def body(step, carry):
            here = pl.ds(pl.multiple_of(step * STEP, STEP), STEP)
            for t in range(tiles):
                value = held[slot, 0, here, pl.ds(t * LANES, LANES)]
                factor = inverse[t : t + 1, :]
                narrow[here, pl.ds(which * width + first + t * LANES, LANES)] = (value * factor).astype(jnp.bfloat16)
            return carry

        lax.fori_loop(0, rows // STEP, body, 0)

    def start(copies):
        for copy in copies:
            copy.start()

    start(first_loads(0))
    start(first_loads(1))
    barrier = pltpu.get_barrier_semaphore()
    for peer in (beside, above, across):
        pl.semaphore_signal(barrier, inc=1, device_id={"shard": peer}, device_id_type=MESH)

    def spread_gain(low, high):
        for b in range(low // LANES, high // LANES):
            gain[pl.ds(b * LANES, LANES), :] = jnp.broadcast_to(gain_rows[b : b + 1, :], (LANES, LANES)).T

    spread_gain(0, HEAD)

    for k in range(count + 1):
        if k < count:
            if k == 0:
                for copy in first_loads(0):
                    copy.wait()
                totals = add_up(0, 0, HEAD, zeros(0))
                pl.semaphore_wait(barrier, 3)

                @pl.when(leads)
                def _():
                    cast_early(0, HEAD)
                    start(send_early(0))

                spread_gain(HEAD, rows)
                for copy in first_loads(1):
                    copy.wait()
                start(loads(1))
                keep_sums(0, add_up(0, HEAD, rows, totals))
            else:
                for copy in loads(k):
                    copy.wait()
                if k == 1:
                    start(loads(2))
                keep_sums(k, add_up(k, 0, rows, zeros(k)))
            start(send_sums(k))
            if k < 2:

                @pl.when(leads)
                def _():
                    if k == 0:
                        cast_early(HEAD, rows)
                    start(send_early(k + 1))

        if k > 0:
            for copy in send_sums(k - 1):
                copy.wait_recv()
            narrow_down(k - 1)
            if k == HOLD:

                @pl.when(jnp.logical_not(leads))
                def _():
                    for early_k in range(HOLD - 1):
                        start(send_own(early_k))

            if 1 < k < HOLD:

                @pl.when(leads)
                def _():
                    start(send_own(k - 1))

            if k >= HOLD:
                start(send_own(k - 1))
            keep_own(k - 1).start()
            if k - 1 + SLOTS < count:
                start(loads(k - 1 + SLOTS))

    for k, (which, _, _, part) in enumerate(chunks):
        if k == 0:

            @pl.when(leads)
            def _():
                for half in range(3):
                    send_early(half)[1].wait_recv()
                early_on().start()

            @pl.when(jnp.logical_not(leads))
            def _():
                send_own(0, (1,))[0].wait_recv()
                send_on(0).start()

        elif part is None:
            send_own(k, (1 - which,))[0].wait_recv()
            send_on(k).start()

    @pl.when(leads)
    def _():
        for half in range(3):
            send_early(half)[0].wait_recv()
        early_on().wait()
        scale_early()
        start(keep_early())
        for half in range(3):
            for copy in send_early(half):
                copy.wait_send()
        for copy in keep_early():
            copy.wait()

    @pl.when(jnp.logical_not(leads))
    def _():
        send_own(0, (0,))[0].wait_recv()
        for copy in send_own(0):
            copy.wait_send()
        send_on(0).wait()

    for k, (which, _, _, part) in enumerate(chunks):
        if k == 0:
            for copy in send_sums(k):
                copy.wait_send()
            keep_own(k).wait()
            continue
        arrived = send_own(k)
        arrived[which].wait_recv()
        if part is not None:
            arrived[1 - which].wait_recv()
        for copy in send_sums(k):
            copy.wait_send()
        for copy in arrived:
            copy.wait_send()
        keep_own(k).wait()
        if part is None:
            send_on(k).wait()


AHEAD = 4
RING = 8


def place_kernel(
    rows,
    width,
    body,
    parts,
    main_gate,
    main_up,
    tail_gate_0,
    tail_gate_1,
    tail_up_0,
    tail_up_1,
    columns_in,
    out_gate,
    out_up,
    columns,
    ring,
    load_sem,
    store_sem,
):
    me = lax.axis_index("shard")
    beside, above, across = places(me)
    columns[...] = columns_in[...]
    high = rows // parts
    jobs = []
    for which, (main, out, tails) in enumerate(
        ((main_gate, out_gate, (tail_gate_0, tail_gate_1)), (main_up, out_up, (tail_up_0, tail_up_1)))
    ):
        for origin, kind in ((me, 0), ((beside, above)[which], 0), ((above, beside)[which], 1), (across, 2)):
            for b in range(parts):
                here = pl.ds(origin * rows + b * high, high)
                pieces = []
                if kind == 0:
                    pieces.append((main.at[here, :], 0, width))
                else:
                    pieces.append((main.at[here, pl.ds(0, body)], 0, body))
                if kind == 1:
                    at = body
                    for tail in tails:
                        size = tail.shape[1]
                        pieces.append((tail.at[pl.ds(b * high, high), :], at, size))
                        at += size
                wide = body if kind == 2 else width
                jobs.append((pieces, out.at[here, pl.ds(0, wide)], wide))

    def load(i):
        slot = i % RING
        return [
            pltpu.make_async_copy(source, ring.at[slot, :, pl.ds(at, size)], load_sem.at[slot, j])
            for j, (source, at, size) in enumerate(jobs[i][0])
        ]

    def store(i):
        slot = i % RING
        _, target, wide = jobs[i]
        return pltpu.make_async_copy(ring.at[slot, :, pl.ds(0, wide)], target, store_sem.at[slot])

    count = len(jobs)
    for i in range(min(AHEAD, count)):
        for copy in load(i):
            copy.start()
    for i in range(count):
        later = i + AHEAD
        if later < count:
            if later >= RING:
                store(later - RING).wait()
            for copy in load(later):
                copy.start()
        for copy in load(i):
            copy.wait()
        store(i).start()
    for i in range(max(0, count - RING), count):
        store(i).wait()


def last_kernel(rows, first, from_gate, from_up, old_gate, old_up, out_gate, out_up, store_sem):
    me = lax.axis_index("shard")
    _, _, across = places(me)
    size = from_gate.shape[1]
    outs = [
        pltpu.make_async_copy(
            source, target.at[pl.ds(across * rows, rows), pl.ds(first, size)], store_sem.at[i]
        )
        for i, (source, target) in enumerate(((from_gate, out_gate), (from_up, out_up)))
    ]
    for copy in outs:
        copy.start()
    for copy in outs:
        copy.wait()


def per_device(w_gate, first_gate, second_gate, w_up, first_up, second_up, norm_gain):
    rows, width = w_gate.shape
    shards = lax.axis_size("shard")
    if shards != 4 or width % LANES or rows % LANES or rows < 3 * HEAD or width // LANES < sum(TAIL) + 4:
        return plain(w_gate, first_gate, second_gate, w_up, first_up, second_up, norm_gain)
    chunks = chunks_of(width // LANES)
    body = width - sum(TAIL) * LANES
    most = max(size for _, _, size, _ in chunks)
    count = len(chunks)
    anywhere = pl.BlockSpec(memory_space=pl.ANY)
    in_vmem = pl.BlockSpec(memory_space=pltpu.VMEM)
    in_hbm = pl.BlockSpec(memory_space=pltpu.HBM)
    dma = pltpu.SemaphoreType.DMA
    whole = jax.ShapeDtypeStruct((shards * rows, width), jnp.bfloat16)
    two = jax.ShapeDtypeStruct((2, width), jnp.float32)
    tails = tuple(jax.ShapeDtypeStruct((rows, size * LANES), jnp.bfloat16) for size in TAIL)
    main_gate, main_up, tg0, tg1, tu0, tu1, columns = pl.pallas_call(
        functools.partial(exchange_kernel, chunks, rows, width),
        name="exchange",
        out_shape=(whole, whole, *tails, *tails, two),
        in_specs=[anywhere] * 6 + [in_vmem],
        out_specs=(anywhere,) * 6 + (in_vmem,),
        scratch_shapes=[
            pltpu.VMEM((SLOTS, 3, rows, most), jnp.float32),
            pltpu.VMEM((rows, 2 * width), jnp.bfloat16),
            pltpu.VMEM((4, count, 8, LANES), jnp.float32),
            pltpu.VMEM((rows, LANES), jnp.float32),
            pltpu.VMEM((rows, LANES), jnp.bfloat16),
            pltpu.VMEM((3, rows, LANES), jnp.bfloat16),
            pltpu.VMEM((3, rows, LANES), jnp.bfloat16),
            dma((SLOTS, 3)),
            dma((count, 3)),
            dma((count, 3)),
            dma((count, 2)),
            dma((count, 2)),
            dma((count,)),
            dma((count,)),
            dma((count,)),
            dma((3, 2)),
            dma((3, 2)),
            dma((2,)),
            dma((3,)),
            dma((2, 3)),
        ],
        compiler_params=pltpu.CompilerParams(
            collective_id=0, has_side_effects=True, vmem_limit_bytes=56 * 1024 * 1024
        ),
    )(w_gate, first_gate, second_gate, w_up, first_up, second_up, norm_gain.reshape(rows // LANES, LANES))
    on = [
        (lax.ppermute(gate, "shard", X_PAIRS), lax.ppermute(up, "shard", Y_PAIRS))
        for gate, up in ((tg0, tu0), (tg1, tu1))
    ]
    parts = 4
    out_gate, out_up, columns = pl.pallas_call(
        functools.partial(place_kernel, rows, width, body, parts),
        name="place",
        out_shape=(whole, whole, two),
        in_specs=[in_hbm] * 6 + [in_vmem],
        out_specs=(anywhere, anywhere, in_vmem),
        scratch_shapes=[
            pltpu.VMEM((RING, rows // parts, width), jnp.bfloat16),
            dma((RING, 3)),
            dma((RING,)),
        ],
        compiler_params=pltpu.CompilerParams(vmem_limit_bytes=VMEM - 2 * sum(TAIL) * LANES * rows * 2 - 256 * 1024),
        cost_estimate=pl.CostEstimate(flops=50_000_000, bytes_accessed=90_000_000, transcendentals=0),
    )(main_gate, main_up, tg0, tg1, tu0, tu1, columns)
    column_gate, column_up = columns[0], columns[1]
    first = body
    for (gate, up), size in zip(on, TAIL):
        out_gate, out_up = pl.pallas_call(
            functools.partial(last_kernel, rows, first),
            name="last",
            out_shape=(whole, whole),
            in_specs=[in_vmem, in_vmem, anywhere, anywhere],
            out_specs=(anywhere, anywhere),
            scratch_shapes=[dma((2,))],
            input_output_aliases={2: 0, 3: 1},
            compiler_params=pltpu.CompilerParams(vmem_limit_bytes=1024 * 1024),
        )(gate, up, out_gate, out_up)
        first += size * LANES
    return (out_gate, out_up, column_gate, column_up)


def solution(mesh):
    return jax.shard_map(
        per_device,
        mesh=mesh,
        in_specs=(
            P("shard", "tp"),
            P("shard", "tp"),
            P("shard", "tp"),
            P("shard", "tp"),
            P("shard", "tp"),
            P("shard", "tp"),
            P("shard"),
        ),
        out_specs=(P(None, "tp"), P(None, "tp"), P("tp"), P("tp")),
        check_vma=False,
    )
```
